32 devices in a mesh: frame: 4 (over x, core), fsdp: 4 (over z), head: 2 (over y).
Axes of the slice: x: 2, y: 2, z: 4, core: 2. Of those that a mesh axis runs over, the one named last changes fastest.
Arguments:
- queries: bfloat16 [1024, 10240], P('frame', ('fsdp', 'head')), may hold values from -6 to 6
- noisy_keys: bfloat16 [1024, 10240], P('frame', ('fsdp', 'head')), may hold values from -6 to 6
- noisy_values: bfloat16 [1024, 10240], P('frame', ('fsdp', 'head')), may hold values from -6 to 6
- clean_keys: bfloat16 [1024, 10240], P('frame', ('fsdp', 'head')), may hold values from -10 to 10
- clean_values: bfloat16 [1024, 10240], P('frame', ('fsdp', 'head')), may hold values from -6 to 6
- gain_query: float32 [5120], replicated, may hold values from 0.5 to 2
- gain_key: float32 [5120], replicated, may hold values from 0.5 to 2
- out_grad: bfloat16 [1024, 10240], P('frame', ('fsdp', 'head')), may hold values from -6 to 6
Outputs:
- attended: bfloat16 [1024, 10240], P('frame', ('fsdp', 'head'))
- grad_queries: bfloat16 [1024, 10240], P('frame', ('fsdp', 'head'))
- grad_keys: bfloat16 [1024, 10240], P('frame', ('fsdp', 'head'))
- grad_values: bfloat16 [1024, 10240], P('frame', ('fsdp', 'head'))
- grad_gain_query: float32 [5120], replicated
- grad_gain_key: float32 [5120], replicated
The draws below stay inside these ranges and needn't reach their ends.
All inputs are finite; a program needn't handle non-finite values.
Results may differ from the reference program's by a relative error of at most 0.012.
Values may be sent and summed in bfloat16 or wider, within the bound.
A program may use at most 64 MiB of HBM per device.

```python
import math
import jax
import jax.numpy as jnp
from jax import lax

D = 5120
HEADS = 40
DH = 128
FRAME_TOK = 256
FRAMES = 4
SEQ = 1024
VIDEOS = 2


def half_scales(key, salt):
    lowest = math.log(0.2)
    drawn = jax.random.uniform(jax.random.fold_in(key, salt), (SEQ, VIDEOS, 2), jnp.float32, lowest, 0.0)
    scales = jnp.exp(drawn)
    columns = jnp.arange(VIDEOS * D)
    video_of = columns % (VIDEOS * D // 2) // (D // 2)
    half_of = columns // (VIDEOS * D // 2)
    return scales[:, video_of, half_of]


def draw_queries(key, part):
    base = jnp.clip(jax.random.normal(jax.random.fold_in(key, 11), (SEQ, VIDEOS * D), jnp.float32), -6.0, 6.0)
    base = base * half_scales(key, 4411)
    return base.astype(jnp.bfloat16)


def draw_noisy_keys(key, part):
    base = jnp.clip(jax.random.normal(jax.random.fold_in(key, 13), (SEQ, VIDEOS * D), jnp.float32), -6.0, 6.0)
    base = base * half_scales(key, 4413)
    return base.astype(jnp.bfloat16)


def draw_clean_keys(key, part):
    base = jnp.clip(jax.random.normal(jax.random.fold_in(key, 12), (SEQ, VIDEOS * D), jnp.float32), -6.0, 6.0)
    return base.astype(jnp.bfloat16)


def block_levels(key, extent, shards, smallest, top_value):
    level = 1.0
    for dim, shards_of in shards:
        draws = jax.random.uniform(jax.random.fold_in(jax.random.fold_in(key, 6), dim), (shards_of,), jnp.float32, smallest / len(shards), top_value / len(shards))
        level = level * jnp.repeat(jnp.exp(draws), extent[dim] // shards_of).reshape((-1,) + (1,) * (len(extent) - 1 - dim))
    return level


def normal_values(rng, extent, width, bound, pieces=(), kind=jnp.bfloat16):
    level = block_levels(rng, extent, pieces, -0.22, 0.18) if pieces else 1.0
    values = jax.random.normal(rng, extent, jnp.float32) * width * level
    return jnp.minimum(jnp.maximum(values, -bound), bound).astype(kind)


def setup_inputs(seed: int = 0) -> dict:
    keys = jax.random.split(jax.random.key(seed), 9)
    queries = draw_queries(jax.random.fold_in(keys[8], 71), 0)
    noisy_keys = draw_noisy_keys(jax.random.fold_in(keys[8], 71), 0)
    noisy_values = normal_values(keys[2], (SEQ, VIDEOS * D), 1.0, 6.0, ((0, 4), (1, 8)))
    clean_keys = draw_clean_keys(jax.random.fold_in(keys[8], 71), 0)
    clean_values = normal_values(keys[4], (SEQ, VIDEOS * D), 1.0, 6.0, ((0, 4), (1, 8)))
    gain_query = jnp.clip(jnp.exp(jax.random.uniform(keys[5], (D,), jnp.float32, math.log(0.5), math.log(2.0))), 0.5, 2.0)
    gain_key = jnp.clip(jnp.exp(jax.random.uniform(keys[6], (D,), jnp.float32, math.log(0.5), math.log(2.0))), 0.5, 2.0)
    out_grad = normal_values(keys[7], (SEQ, VIDEOS * D), 1.0, 6.0, ((0, 4), (1, 8)))
    return {"queries": queries, "noisy_keys": noisy_keys, "noisy_values": noisy_values, "clean_keys": clean_keys, "clean_values": clean_values, "gain_query": gain_query, "gain_key": gain_key, "out_grad": out_grad}


EPSILON = 1e-06

def rounded(values_in):
    return lax.optimization_barrier(values_in.astype(jnp.bfloat16)).astype(jnp.float32)

def normalize(raw, gain):
    full = raw.astype(jnp.float32)
    rate = lax.rsqrt(lax.optimization_barrier(jnp.mean(full * full, axis=1)) + EPSILON)
    return (full, rate, (full * rate[:, None] * gain).astype(jnp.bfloat16))

def norm_grad(full, rate, gain, grad_normed):
    flat = grad_normed * gain
    inner = lax.optimization_barrier(jnp.sum(full * flat, axis=1))
    grad_raw = rate[:, None] * flat - full * (rate * rate * rate * inner / D)[:, None]
    grad_gain = lax.optimization_barrier(jnp.sum(grad_normed * full * rate[:, None], axis=0))
    return (grad_raw.astype(jnp.bfloat16), grad_gain)

def by_video(array):
    split = array.reshape(SEQ, 2, VIDEOS, D // 2)
    return jnp.transpose(split, (2, 0, 1, 3)).reshape(VIDEOS, SEQ, D)

def by_column(array):
    split = array.reshape(VIDEOS, SEQ, 2, D // 2)
    return jnp.transpose(split, (1, 2, 0, 3)).reshape(SEQ, VIDEOS * D)

def reference(queries, noisy_keys, noisy_values, clean_keys, clean_values, gain_query, gain_key, out_grad):
    scaling = 1.0 / math.sqrt(DH)
    highest = lax.Precision.HIGHEST

    def one_video(inputs):
        video_q, video_k, video_v, video_ck, video_cv, video_g = inputs
        q_full, rate_q, normed_q = normalize(video_q, gain_query)
        k_full, rate_k, normed_k = normalize(video_k, gain_key)
        outputs, grads_q, grads_k, grads_v = ([], [], [], [])
        for frame_index in range(FRAMES):
            first_row = frame_index * FRAME_TOK
            last_row = first_row + FRAME_TOK
            query_f = normed_q[first_row:last_row].astype(jnp.float32).reshape(FRAME_TOK, HEADS, DH)
            key_all = jnp.concatenate([normed_k[first_row:last_row], video_ck[:first_row]], axis=0)
            key_all = key_all.astype(jnp.float32).reshape(-1, HEADS, DH)
            value_all = jnp.concatenate([video_v[first_row:last_row], video_cv[:first_row]], axis=0)
            value_all = value_all.astype(jnp.float32).reshape(-1, HEADS, DH)
            grad_out = video_g[first_row:last_row].astype(jnp.float32).reshape(FRAME_TOK, HEADS, DH)
            scores = jnp.einsum('qhd,khd->hqk', query_f, key_all, precision=highest) * scaling
            row_max = lax.optimization_barrier(jnp.max(scores, axis=2))
            expo = jnp.exp(scores - row_max[:, :, None])
            total = lax.optimization_barrier(jnp.sum(expo, axis=2))
            summed = jnp.einsum('hqk,khd->qhd', rounded(expo), value_all, precision=highest)
            attention_f32 = summed / jnp.transpose(total)[:, :, None]
            log_total = row_max + jnp.log(total)
            soft_probs = jnp.exp(scores - log_total[:, :, None])
            delta = jnp.transpose(lax.optimization_barrier(jnp.sum(grad_out * attention_f32, axis=2)))
            grad_probs = jnp.einsum('qhd,khd->hqk', grad_out, value_all, precision=highest)
            grad_scores = rounded(soft_probs * (grad_probs - delta[:, :, None]))
            grad_qn = jnp.einsum('hqk,khd->qhd', grad_scores, key_all, precision=highest) * scaling
            grad_kn = jnp.einsum('hqk,qhd->khd', grad_scores[:, :, :FRAME_TOK], query_f, precision=highest) * scaling
            grad_vv = jnp.einsum('hqk,qhd->khd', rounded(soft_probs[:, :, :FRAME_TOK]), grad_out, precision=highest)
            outputs.append(attention_f32.reshape(FRAME_TOK, D).astype(jnp.bfloat16))
            grads_q.append(grad_qn.reshape(FRAME_TOK, D))
            grads_k.append(grad_kn.reshape(FRAME_TOK, D))
            grads_v.append(grad_vv.reshape(FRAME_TOK, D).astype(jnp.bfloat16))
        grad_q_raw, gain_q_part = norm_grad(q_full, rate_q, gain_query, jnp.concatenate(grads_q, axis=0))
        grad_k_raw, gain_k_part = norm_grad(k_full, rate_k, gain_key, jnp.concatenate(grads_k, axis=0))
        return (jnp.concatenate(outputs, axis=0), grad_q_raw, grad_k_raw, jnp.concatenate(grads_v, axis=0), gain_q_part, gain_k_part)
    stacked = tuple((by_video(member) for member in (queries, noisy_keys, noisy_values, clean_keys, clean_values, out_grad)))
    results = lax.map(one_video, stacked)
    attended, grad_queries, grad_keys, grad_values, gain_q_parts, gain_k_parts = results
    return (by_column(attended), by_column(grad_queries), by_column(grad_keys), by_column(grad_values), lax.optimization_barrier(jnp.sum(gain_q_parts, axis=0)), lax.optimization_barrier(jnp.sum(gain_k_parts, axis=0)))
```

```python
import functools
import math

import jax
import jax.numpy as jnp
from jax import lax
from jax.experimental import pallas as pl
from jax.experimental.pallas import tpu as pltpu
from jax.sharding import PartitionSpec as P

DH = 128
EPSILON = 1e-06
MESH = pl.DeviceIdType.MESH
F32 = jnp.float32
BF16 = jnp.bfloat16


def dot_nt(a, b):
    return lax.dot_general(a, b, (((1,), (1,)), ((), ())), preferred_element_type=F32)


def dot_nn(a, b):
    return lax.dot_general(a, b, (((1,), (0,)), ((), ())), preferred_element_type=F32)


def dot_tn(a, b):
    return lax.dot_general(a, b, (((0,), (0,)), ((), ())), preferred_element_type=F32)


def kernel(
    frames, fsdp, heads_axis, width, features,
    q_hbm, k_hbm, v_hbm, ck_hbm, cv_hbm, gq_hbm, gk_hbm, g_hbm,
    att_out, dq_out, dk_out, dv_out, gain_q_out, gain_k_out,
    q, k, v, g, gq, gk, cks, cvs, flat_q, flat_k, inner_q, inner_k, rates,
    stats, sums1, sums2,
    load_sem, own_send, relay_send, clean_recv, stats_send, stats_recv, s1_send, s1_recv, s2_send, s2_recv,
):
    length = q.shape[0]
    head_count = width // DH
    videos = fsdp // 2
    scaling = 1.0 / math.sqrt(DH)
    power = scaling * math.log2(math.e)
    frame = lax.axis_index("frame")
    fs = lax.axis_index("fsdp")
    half = fs // videos
    video = lax.rem(fs, videos)
    me1 = frame * videos + video
    n1 = frames * videos
    me2 = half * heads_axis + lax.axis_index("head")
    n2 = 2 * heads_axis

    def peer1(distance):
        p = lax.rem(me1 + distance, n1)
        return {"frame": p // videos, "fsdp": half * videos + lax.rem(p, videos)}

    def peer2(distance):
        p = lax.rem(me2 + distance, n2)
        return {"fsdp": (p // heads_axis) * videos + video, "head": lax.rem(p, heads_axis)}

    barrier = pltpu.get_barrier_semaphore()

    def greet(d, _):
        pl.semaphore_signal(barrier, inc=1, device_id=peer1(d), device_id_type=MESH)
        return 0

    lax.fori_loop(1, n1, greet, 0)
    for d in range(1, n2):
        pl.semaphore_signal(barrier, inc=1, device_id=peer2(d), device_id_type=MESH)
    start = pl.multiple_of(me2 * width, DH)
    loads = []
    for i, (src, dst) in enumerate(
        (
            (q_hbm, q),
            (k_hbm, k),
            (gq_hbm.at[:, pl.ds(start, width)], gq),
            (gk_hbm.at[:, pl.ds(start, width)], gk),
            (v_hbm, v),
            (g_hbm, g),
        )
    ):
        copy = pltpu.make_async_copy(src, dst, load_sem.at[i])
        copy.start()
        loads.append(copy)
    pl.semaphore_wait(barrier, n1 - 1 + n2 - 1)

    def columns(h):
        return pl.ds(pl.multiple_of(h * DH, DH), DH)

    def clean_copy(j, h, kv, target, sends, own):
        cols = columns(h)
        land = (cks, cvs)[kv].at[j, :, cols]
        src = (ck_hbm, cv_hbm)[kv].at[:, cols] if own else land
        return pltpu.make_async_remote_copy(
            src_ref=src,
            dst_ref=land,
            send_sem=sends.at[h, kv],
            recv_sem=clean_recv.at[j, h, kv],
            device_id={"frame": jnp.int32(target)},
            device_id_type=MESH,
        )

    def plan(nb):
        pair, side = nb // 2, nb % 2
        partner, further = 2 * pair + 1 - side, nb + 2
        direct = [2 * c + side for c in range(pair)]
        relayed = [2 * c + 1 - side for c in range(pair)] + ([nb - 1] if side else [])
        own = ([further] if further < frames else []) + ([partner] if side == 0 else [])
        passes = [partner] + ([further] if further < frames else [])
        return direct, relayed, own, passes

    for nb in range(frames):
        _, _, own, _ = plan(nb)
        if own:

            @pl.when(frame == nb)
            def _():
                def go(h, _):
                    for t, target in enumerate(own):
                        for kv in range(2):
                            clean_copy(nb, h, kv, target, own_send.at[t], True).start()
                    return 0

                lax.fori_loop(0, head_count, go, 0)

    row = lax.broadcasted_iota(jnp.int32, (8, length), 0)

    def as_rows(a, b):
        a = jnp.sum(jnp.transpose(a), axis=0, keepdims=True)
        b = jnp.sum(jnp.transpose(b), axis=0, keepdims=True)
        return jnp.where(row == 0, a, jnp.where(row == 1, b, 0.0))

    def stats_copy(phase, d, slot):
        return pltpu.make_async_remote_copy(
            src_ref=stats.at[phase, slot],
            dst_ref=stats.at[phase, slot],
            send_sem=stats_send.at[phase, d],
            recv_sem=stats_recv.at[phase, d],
            device_id=peer2(d),
            device_id_type=MESH,
        )

    def stats_go(phase, value):
        stats[phase, me2] = value
        for d in range(1, n2):
            stats_copy(phase, d, me2).start()

    def stats_total(phase):
        for d in range(1, n2):
            stats_copy(phase, d, lax.rem(me2 + n2 - d, n2)).wait_recv()
        return jnp.sum(stats[phase], axis=0)

    loads[0].wait()
    loads[1].wait()

    def square(ref):
        total = jnp.zeros((length, DH), F32)
        for h in range(head_count):
            x = ref[:, h * DH : (h + 1) * DH].astype(F32)
            total = total + x * x
        return total

    stats_go(0, as_rows(square(q), square(k)))
    inner_q[...] = jnp.zeros_like(inner_q)
    inner_k[...] = jnp.zeros_like(inner_k)
    for copy in loads[2:]:
        copy.wait()
    rates[...] = jnp.transpose(lax.rsqrt(stats_total(0) / features + EPSILON))

    def head_step(nb, h):
        direct, relayed, _, passes = plan(nb)
        cols = columns(h)
        for j in direct:
            for kv in range(2):
                clean_copy(j, h, kv, passes[0], relay_send.at[0, j], False).wait_recv()
                for t, target in enumerate(passes):
                    clean_copy(j, h, kv, target, relay_send.at[t, j], False).start()
        rate_q = rates[:, 0:1]
        rate_k = rates[:, 1:2]
        q_full = q[:, cols].astype(F32)
        k_full = k[:, cols].astype(F32)
        gain_q = gq[:, cols]
        gain_k = gk[:, cols]
        qn = (q_full * rate_q * gain_q).astype(BF16)
        kn = (k_full * rate_k * gain_k).astype(BF16)
        val = v[:, cols]
        grad = g[:, cols]
        scores = [dot_nt(qn, kn)]
        grad_probs = [dot_nt(grad, val)]
        for j in relayed:
            for kv in range(2):
                clean_copy(j, h, kv, passes[0], relay_send.at[0, j], False).wait_recv()
        for j in range(nb):
            scores.append(dot_nt(qn, cks[j, :, cols]))
            grad_probs.append(dot_nt(grad, cvs[j, :, cols]))
        top = functools.reduce(jnp.maximum, [jnp.max(s, axis=1, keepdims=True) for s in scores])
        expo = [jnp.exp2((s - top) * power) for s in scores]
        total = functools.reduce(jnp.add, [jnp.sum(e, axis=1, keepdims=True) for e in expo])
        summed = dot_nn(expo[0].astype(BF16), val)
        for j in range(nb):
            summed = summed + dot_nn(expo[j + 1].astype(BF16), cvs[j, :, cols])
        inverse = 1.0 / total
        attention = summed * inverse
        att_out[:, cols] = attention.astype(BF16)
        delta = jnp.sum(grad.astype(F32) * attention, axis=1, keepdims=True)
        probs = [e * inverse for e in expo]
        grad_scores = [(p * (d - delta)).astype(BF16) for p, d in zip(probs, grad_probs)]
        grad_qn = dot_nn(grad_scores[0], kn)
        for j in range(nb):
            grad_qn = grad_qn + dot_nn(grad_scores[j + 1], cks[j, :, cols])
        grad_qn = grad_qn * scaling
        grad_kn = dot_tn(grad_scores[0], qn) * scaling
        dv_out[:, cols] = dot_tn(probs[0].astype(BF16), grad).astype(BF16)
        fq = grad_qn * gain_q
        fk = grad_kn * gain_k
        flat_q[:, cols] = fq
        flat_k[:, cols] = fk
        inner_q[...] += q_full * fq
        inner_k[...] += k_full * fk
        sums1[me1, 0:1, cols] = jnp.sum(grad_qn * q_full * rate_q, axis=0, keepdims=True)
        sums1[me1, 1:2, cols] = jnp.sum(grad_kn * k_full * rate_k, axis=0, keepdims=True)

    for nb in range(frames):

        @pl.when(frame == nb)
        def _():
            def step(h, _):
                head_step(nb, h)
                return 0

            lax.fori_loop(0, head_count, step, 0)

    stats_go(1, as_rows(inner_q[...], inner_k[...]))

    def s1_copy(d, slot):
        return pltpu.make_async_remote_copy(
            src_ref=sums1.at[slot],
            dst_ref=sums1.at[slot],
            send_sem=s1_send.at[d],
            recv_sem=s1_recv.at[d],
            device_id=peer1(d),
            device_id_type=MESH,
        )

    def s2_copy(d, slot):
        return pltpu.make_async_remote_copy(
            src_ref=sums2.at[slot],
            dst_ref=sums2.at[slot],
            send_sem=s2_send.at[d],
            recv_sem=s2_recv.at[d],
            device_id=peer2(d),
            device_id_type=MESH,
        )

    def s1_go(d, _):
        s1_copy(d, me1).start()
        return 0

    lax.fori_loop(1, n1, s1_go, 0)

    inners = jnp.transpose(stats_total(1))
    rate_q = rates[:, 0:1]
    rate_k = rates[:, 1:2]
    cube_q = rate_q * rate_q * rate_q * inners[:, 0:1] / features
    cube_k = rate_k * rate_k * rate_k * inners[:, 1:2] / features

    def s1_land(d, _):
        s1_copy(d, lax.rem(me1 + n1 - d, n1)).wait_recv()
        return 0

    lax.fori_loop(1, n1, s1_land, 0)
    sums2[me2] = jnp.sum(sums1[...], axis=0)
    for d in range(1, n2):
        s2_copy(d, me2).start()

    def finish(h, _):
        cols = columns(h)
        dq_out[:, cols] = (rate_q * flat_q[:, cols] - q[:, cols].astype(F32) * cube_q).astype(BF16)
        dk_out[:, cols] = (rate_k * flat_k[:, cols] - k[:, cols].astype(F32) * cube_k).astype(BF16)
        return 0

    lax.fori_loop(0, head_count, finish, 0)
    for d in range(1, n2):
        s2_copy(d, lax.rem(me2 + n2 - d, n2)).wait_recv()
    for p in range(n2):
        gain_q_out[:, p * width : (p + 1) * width] = sums2[p, 0:1, :]
        gain_k_out[:, p * width : (p + 1) * width] = sums2[p, 1:2, :]

    for d in range(1, n2):
        stats_copy(0, d, me2).wait_send()
        stats_copy(1, d, me2).wait_send()
        s2_copy(d, me2).wait_send()

    def s1_gone(d, _):
        s1_copy(d, me1).wait_send()
        return 0

    lax.fori_loop(1, n1, s1_gone, 0)
    for nb in range(frames):
        direct, _, own, passes = plan(nb)

        @pl.when(frame == nb)
        def _():
            def gone(h, _):
                for kv in range(2):
                    for t, target in enumerate(own):
                        clean_copy(nb, h, kv, target, own_send.at[t], True).wait_send()
                    for j in direct:
                        for t, target in enumerate(passes):
                            clean_copy(j, h, kv, target, relay_send.at[t, j], False).wait_send()
                return 0

            lax.fori_loop(0, head_count, gone, 0)


def on_device(queries, noisy_keys, noisy_values, clean_keys, clean_values, gain_query, gain_key, out_grad):
    length, width = queries.shape
    features = gain_query.shape[0]
    frames = lax.axis_size("frame")
    fsdp = lax.axis_size("fsdp")
    heads_axis = lax.axis_size("head")
    head_count = width // DH
    n1 = frames * (fsdp // 2)
    n2 = 2 * heads_axis
    block = jax.ShapeDtypeStruct((length, width), BF16)
    gains = jax.ShapeDtypeStruct((1, features), F32)
    anywhere = pl.BlockSpec(memory_space=pl.ANY)
    vmem = pl.BlockSpec(memory_space=pltpu.VMEM)
    dma = pltpu.SemaphoreType.DMA
    earlier = max(frames - 1, 1)
    outs = pl.pallas_call(
        functools.partial(kernel, frames, fsdp, heads_axis, width, features),
        out_shape=(block, block, block, block, gains, gains),
        in_specs=[anywhere] * 8,
        out_specs=[vmem] * 6,
        scratch_shapes=[
            pltpu.VMEM((length, width), BF16),
            pltpu.VMEM((length, width), BF16),
            pltpu.VMEM((length, width), BF16),
            pltpu.VMEM((length, width), BF16),
            pltpu.VMEM((1, width), F32),
            pltpu.VMEM((1, width), F32),
            pltpu.VMEM((earlier, length, width), BF16),
            pltpu.VMEM((earlier, length, width), BF16),
            pltpu.VMEM((length, width), F32),
            pltpu.VMEM((length, width), F32),
            pltpu.VMEM((length, DH), F32),
            pltpu.VMEM((length, DH), F32),
            pltpu.VMEM((length, 8), F32),
            pltpu.VMEM((2, n2, 8, length), F32),
            pltpu.VMEM((n1, 2, width), F32),
            pltpu.VMEM((n2, 2, width), F32),
            dma((6,)),
            dma((2, head_count, 2)),
            dma((2, earlier, head_count, 2)),
            dma((earlier, head_count, 2)),
            dma((2, n2)),
            dma((2, n2)),
            dma((n1,)),
            dma((n1,)),
            dma((n2,)),
            dma((n2,)),
        ],
        compiler_params=pltpu.CompilerParams(collective_id=0, has_side_effects=True),
        name="attention",
    )(
        queries, noisy_keys, noisy_values, clean_keys, clean_values,
        gain_query.reshape(1, features), gain_key.reshape(1, features), out_grad,
    )
    return (*outs[:4], outs[4].reshape(features), outs[5].reshape(features))


def solution(mesh):
    tokens = P("frame", ("fsdp", "head"))
    return jax.shard_map(
        on_device,
        mesh=mesh,
        in_specs=(tokens, tokens, tokens, tokens, tokens, P(), P(), tokens),
        out_specs=(tokens, tokens, tokens, tokens, P(), P()),
        check_vma=False,
    )
```
